256 devices in a mesh: ka: 128 (over z, y, x_hi, core), ga: 2 (over x_lo).
Axes of the slice: x: 4 (x_hi: 2, x_lo: 2; x = x_hi * 2 + x_lo), y: 4, z: 8, core: 2. Of those that a mesh axis runs over, the one named last changes fastest.
Arguments:
- coeffs: bfloat16 [128, 240, 2, 64, 128], P('ka', 'ga'), may hold values from -0.44921875 to 0.44921875
- neighbour: int32 [128, 3], P('ka'), may hold values from 0 to 127, as said below
- shift_id: int32 [128, 3], P('ka'), may hold values from 0 to 7
- block_map: int32 [8, 240], replicated, may hold values from 0 to 239, as said below
Outputs:
- intersection: float32 [128, 3, 2, 64, 64], P('ka', None, None, 'ga')
The draws below stay inside these ranges and needn't reach their ends.
Inputs may be any that keep to these rules, and one draw needn't show every extreme that they name: `neighbour`: the k-points are numbered helically. The three columns of row k hold (k + 1) mod 128, (k + 16) mod 128 and (k + 64) mod 128, in an order drawn for each row. `block_map`: each row is a permutation of the 240 blocks. Block j lies in G-slice j // 120. In every row, each G-slice receives exactly 20 of its blocks from one other G-slice, exactly 10 from each of the remaining other G-slices, and the rest from itself.
All inputs are finite; a program needn't handle non-finite values.
Results may differ from the reference program's by a relative error of at most 0.0003.
Values may be sent and summed in bfloat16 or wider, within the bound.
No kernel may reach another device: no remote copies, remote signals or barrier semaphores. Data moves between devices by JAX's collectives and lax.ppermute only.
A program may use at most 128 MiB of HBM per device.

```python
import jax
import jax.numpy as jnp
from jax import lax

NB = 64
NBV = 3
NSHIFT = 8
K_DEV = 1
KPTS = 128
MZ = 16
NBLK = 240
BLK_SL = 120
CAP = 20
N_KA = 128
N_GA = 2


def column_order(one_key):
    return jax.random.permutation(one_key, 3).astype(jnp.int32)


def draw_neighbour(key, part):
    total = K_DEV * N_KA
    points = jnp.arange(total, dtype=jnp.int32)
    z_step = jnp.mod(points + 1, total)
    y_step = jnp.mod(points + MZ, total)
    x_step = jnp.mod(points + total // 2, total)
    stacked = jnp.stack([z_step, y_step, x_step], axis=1).astype(jnp.int32)
    orders = jax.vmap(column_order)(jax.random.split(jax.random.fold_in(key, 17), total))
    return jnp.take_along_axis(stacked, orders, axis=1).astype(jnp.int32)


def row_shuffle(one_key):
    return jax.random.permutation(one_key, BLK_SL).astype(jnp.int32)


def one_map(key):
    keys = jax.random.split(key, 3)
    lighter = CAP // 2
    heavy = jax.random.randint(keys[0], (), 1, N_GA, dtype=jnp.int32)
    rows = jnp.arange(N_GA, dtype=jnp.int32)[:, None]
    cols = jnp.arange(BLK_SL, dtype=jnp.int32)[None, :]
    self_count = BLK_SL - CAP - (N_GA - 2) * lighter
    remain = jnp.maximum(cols - self_count - CAP, 0) // lighter
    other_step = jnp.where(remain + 1 < heavy, remain + 1, remain + 2)
    offset = jnp.where(cols < self_count, 0, jnp.where(cols < self_count + CAP, heavy, other_step))
    labels = jnp.mod(rows + offset, N_GA).astype(jnp.int32)
    shuffles = jax.vmap(row_shuffle)(jax.random.split(keys[1], N_GA))
    labels = jnp.take_along_axis(labels, shuffles, axis=1).reshape(-1)
    grouped = jnp.argsort(labels, stable=True).astype(jnp.int32)
    inner = jax.vmap(row_shuffle)(jax.random.split(keys[2], N_GA))
    sources = (jnp.arange(N_GA, dtype=jnp.int32)[:, None] * BLK_SL + inner).reshape(-1)
    return jnp.zeros((N_GA * BLK_SL,), jnp.int32).at[grouped].set(sources)


def draw_block_map(key, part):
    keys = jax.random.split(key, NSHIFT)
    return jax.vmap(one_map)(keys).astype(jnp.int32)


def place_ends(values, own_key, least, top_value):
    place = [jax.random.randint(jax.random.fold_in(own_key, axis), (), 0, length) for axis, length in enumerate(values.shape)]
    main_axis = values.shape.index(max(values.shape))
    beside = place[:main_axis] + [(place[main_axis] + 1) % values.shape[main_axis]] + place[main_axis + 1:]
    return values.at[tuple(place)].set(least).at[tuple(beside)].set(top_value)


def block_scale(own_key, shape, pieces, smallest, largest):
    factor_of = 1.0
    for position, parts in pieces:
        steps = jax.random.uniform(jax.random.fold_in(jax.random.fold_in(own_key, 6), position), (parts,), jnp.float32, smallest / len(pieces), largest / len(pieces))
        factor_of = factor_of * jnp.repeat(jnp.exp(steps), shape[position] // parts).reshape((-1,) + (1,) * (len(shape) - 1 - position))
    return factor_of


def gaussian(key, extent, deviation, bound, cuts=(), held_as=jnp.bfloat16):
    loudness = block_scale(key, extent, cuts, -0.22, 0.18) if cuts else 1.0
    entries = jax.random.normal(key, extent, jnp.float32) * deviation * loudness
    return jnp.minimum(jnp.maximum(entries, -bound), bound).astype(held_as)


def setup_inputs(seed: int = 0) -> dict:
    arg_keys = jax.random.split(jax.random.key(seed), 5)
    coeffs = gaussian(arg_keys[0], (KPTS, NBLK, 2, NB, 128), 0.0755, 0.44921875, ((0, 128), (1, 2)))
    neighbour = draw_neighbour(jax.random.fold_in(arg_keys[4], 71), 0)
    shift_id = place_ends(jax.random.randint(arg_keys[2], (KPTS, NBV), 0, NSHIFT), jax.random.fold_in(arg_keys[2], 1), 0, NSHIFT - 1).astype(jnp.int32)
    block_map = draw_block_map(jax.random.fold_in(arg_keys[4], 71), 0)
    return dict(coeffs=coeffs, neighbour=neighbour, shift_id=shift_id, block_map=block_map)


def pair_product(left, right):
    return jnp.einsum("jmw,jnw->mn", left, right, precision=lax.Precision.HIGHEST)


def reference(coeffs, neighbour, shift_id, block_map):
    bra_points = (jnp.arange(KPTS * NBV, dtype=jnp.int32) // NBV).astype(jnp.int32)
    ket_points = neighbour.reshape(-1).astype(jnp.int32)
    shifts_flat = shift_id.reshape(-1).astype(jnp.int32)

    def one_pair(inputs):
        bra_point, ket_point, shift_row = inputs
        bra = coeffs[bra_point].astype(jnp.float32)
        ket = jnp.take(coeffs[ket_point], block_map[shift_row], axis=0).astype(jnp.float32)
        real_part = pair_product(bra[:, 0], ket[:, 0]) + pair_product(bra[:, 1], ket[:, 1])
        imag_part = pair_product(bra[:, 0], ket[:, 1]) - pair_product(bra[:, 1], ket[:, 0])
        return jnp.stack([real_part, imag_part])

    result = lax.map(one_pair, (bra_points, ket_points, shifts_flat))
    return result.reshape(KPTS, NBV, 2, NB, NB)
```

```python
import jax
import jax.numpy as jnp
from jax import lax
from jax.experimental import pallas as pl
from jax.experimental.pallas import tpu as pltpu
from jax.sharding import PartitionSpec as P

AXES = ("ka", "ga")
PLANE = 16
UNROLL = 12


def gather_kernel(counts, index_ref, source_ref, *refs):
    outs, sems = refs[: len(counts)], refs[len(counts)]
    first = 0
    for slot, (out, count) in enumerate(zip(outs, counts)):

        def send(n, carry, out=out, place=first, slot=slot):
            pltpu.make_async_copy(
                source_ref.at[index_ref[place + n]], out.at[n], sems.at[slot]
            ).start()
            return carry

        lax.fori_loop(0, count, send, 0)
        first += count
    for slot, (out, count) in enumerate(zip(outs, counts)):
        pltpu.make_async_copy(source_ref.at[pl.ds(0, count)], out, sems.at[slot]).wait()


def gather_blocks(source, index, counts):
    anywhere = pl.BlockSpec(memory_space=pl.ANY)
    return pl.pallas_call(
        lambda *refs: gather_kernel(counts, *refs),
        grid_spec=pltpu.PrefetchScalarGridSpec(
            num_scalar_prefetch=1,
            grid=(),
            in_specs=[anywhere],
            out_specs=[anywhere for _ in counts],
            scratch_shapes=[pltpu.SemaphoreType.DMA((len(counts),))],
        ),
        out_shape=[jax.ShapeDtypeStruct((n,) + source.shape[1:], source.dtype) for n in counts],
        name="gather_blocks",
    )(index, source)


def contract_kernel(sizes, tasks, terms, bra_ref, ket_ref, *refs):
    count = len(sizes)
    sources, out_ref, blocks, sems = refs[:count], refs[count], refs[count + 1], refs[count + 2]
    copies = []
    first = 0
    for slot, size in enumerate(sizes):
        copies.append(
            pltpu.make_async_copy(sources[slot], blocks.at[pl.ds(first, size)], sems.at[slot])
        )
        first += size
    for copy in copies:
        copy.start()
    for copy in copies:
        copy.wait()
    both = blocks.shape[1]
    bands = both // 2
    for task in range(tasks):

        def step(n, total, task=task):
            base = task * terms + n * UNROLL
            bra = jnp.concatenate([blocks[bra_ref[base + u]] for u in range(UNROLL)], axis=1)
            ket = jnp.concatenate([blocks[ket_ref[base + u]] for u in range(UNROLL)], axis=1)
            return total + lax.dot_general(
                bra, ket, (((1,), (1,)), ((), ())), preferred_element_type=jnp.float32
            )

        total = lax.fori_loop(0, terms // UNROLL, step, jnp.zeros((both, both), jnp.float32))
        out_ref[task, 0] = total[:bands, :bands] + total[bands:, bands:]
        out_ref[task, 1] = total[:bands, bands:] - total[bands:, :bands]


def contract(bra_index, ket_index, sources):
    tasks, terms = bra_index.shape
    sizes = [source.shape[0] for source in sources]
    block = sources[0].shape[1:]
    bands = block[0] // 2
    anywhere = pl.BlockSpec(memory_space=pl.ANY)
    return pl.pallas_call(
        lambda *refs: contract_kernel(sizes, tasks, terms, *refs),
        grid_spec=pltpu.PrefetchScalarGridSpec(
            num_scalar_prefetch=2,
            grid=(),
            in_specs=[anywhere for _ in sources],
            out_specs=pl.BlockSpec(memory_space=pltpu.VMEM),
            scratch_shapes=[
                pltpu.VMEM((sum(sizes),) + block, sources[0].dtype),
                pltpu.SemaphoreType.DMA((len(sizes),)),
            ],
        ),
        out_shape=jax.ShapeDtypeStruct((tasks, 2, bands, bands), jnp.float32),
        name="contract",
    )(bra_index.reshape(-1), ket_index.reshape(-1), *sources)


def compact(flag, value, count):
    size = flag.shape[1]
    earlier = jnp.arange(size)[:, None] < jnp.arange(size)[None, :]
    rank = jnp.sum(flag[:, :, None] & earlier[None], axis=1, dtype=jnp.int32)
    hit = flag[:, None, :] & (rank[:, None, :] == jnp.arange(count)[None, :, None])
    return jnp.sum(jnp.where(hit, value[:, None, :], 0), axis=2, dtype=jnp.int32)


def on_device(coeffs, neighbour, shift_id, block_map):
    slab = coeffs.shape[1]
    bands, lanes = coeffs.shape[3], coeffs.shape[4]
    points, slices = lax.axis_size("ka"), lax.axis_size("ga")
    capacity = slab // 6
    k = lax.axis_index("ka")
    g = lax.axis_index("ga")
    plane_place = k % PLANE
    last = plane_place == PLANE - 1
    upward = k % 2 == 1
    stationary = (k < points // 2) == upward
    half = points // 2

    def route(target):
        pairs = []
        for point in range(points):
            for side in range(slices):
                to = target(point, side)
                if to is not None:
                    pairs.append((point * slices + side, to[0] % points * slices + to[1]))
        return pairs

    def move(array, target):
        return lax.ppermute(array, AXES, route(target))

    def moves_far(point):
        return (point < half) == (point % 2 == 0)

    own = coeffs.reshape(slab, 2 * bands, lanes)
    near = move(own, lambda p, s: (p + PLANE if p % 2 else p - PLANE, s))
    far = move(own, lambda p, s: (p + half, s) if moves_far(p) else None)
    ring = move(own, lambda p, s: (p // PLANE * PLANE + (p - 1) % PLANE, s))

    aims = jnp.stack([(k + step) % points for step in (1, PLANE, half)])
    is_aim = neighbour[0][:, None] == aims[None, :]
    shifts = jnp.sum(jnp.where(is_aim, shift_id[0][:, None], 0), axis=0, dtype=jnp.int32)
    shifts_below = move(shifts, lambda p, s: (p + PLANE, s))
    shifts_before = move(shifts, lambda p, s: (p + 1, s))
    shifts_far = move(shifts, lambda p, s: (p + half, s))
    rows = jnp.stack(
        [
            jnp.where(last, shifts_below[0], shifts[0]),
            jnp.where(upward, shifts_below[1], shifts[1]),
            shifts[2],
            shifts_far[2],
            shifts_before[0],
        ]
    )
    picked = rows[:, None] == jnp.arange(block_map.shape[0])[None, :]
    relabel = jnp.sum(jnp.where(picked[:, :, None], block_map[None], 0), axis=1, dtype=jnp.int32)
    dest = jnp.broadcast_to(jnp.arange(relabel.shape[1], dtype=jnp.int32), relabel.shape)
    here, there = dest // slab == g, relabel // slab == g
    dest_local, source_local = dest - g * slab, relabel - g * slab
    outward = compact(here & ~there, dest_local, capacity)
    inward = compact(~here & there, source_local, capacity)
    local_bra = compact(here & there, dest_local, slab - capacity)
    local_ket = compact(here & there, source_local, slab - capacity)

    payload = jnp.concatenate(
        [
            outward[0],
            jnp.where(upward, inward[1], outward[1]),
            outward[2],
            inward[3],
            inward[4],
        ]
    )
    pay_one, pay_plane, pay_far, pay_wrap = gather_blocks(
        own, payload, (capacity, capacity, 2 * capacity, capacity)
    )
    cross_one = move(pay_one, lambda p, s: (p, 1 - s) if p % PLANE != PLANE - 1 else None)
    cross_plane = move(pay_plane, lambda p, s: (p, 1 - s))
    cross_far = move(pay_far, lambda p, s: None if moves_far(p) else (p, 1 - s))
    cross_wrap = move(
        pay_wrap, lambda p, s: (p + PLANE - 1, 1 - s) if p % PLANE == 0 else None
    )

    spots = jnp.arange(capacity, dtype=jnp.int32)
    at_near, at_ring, at_one = slab, 2 * slab, 3 * slab
    at_wrap, at_plane = at_one + capacity, at_one + 2 * capacity
    bra_one = jnp.concatenate(
        [
            local_bra[0] + jnp.where(last, at_near, 0),
            jnp.where(last, at_near + outward[0], at_one + spots),
        ]
    )
    ket_one = jnp.concatenate(
        [at_ring + local_ket[0], jnp.where(last, at_wrap + spots, at_ring + inward[0])]
    )
    bra_plane = jnp.concatenate(
        [
            local_bra[1] + jnp.where(upward, at_near, 0),
            jnp.where(upward, at_near + outward[1], at_plane + spots),
        ]
    )
    ket_plane = jnp.concatenate(
        [
            local_ket[1] + jnp.where(upward, 0, at_near),
            jnp.where(upward, at_plane + spots, at_near + inward[1]),
        ]
    )
    first = contract(
        jnp.stack([bra_one, bra_plane]),
        jnp.stack([ket_one, ket_plane]),
        [own, near, ring, cross_one, cross_wrap, cross_plane],
    )
    at_far, at_cross = slab, 2 * slab
    bra_far = jnp.stack(
        [
            jnp.concatenate([local_bra[2], at_cross + spots]),
            jnp.concatenate([at_far + local_bra[3], at_far + outward[3]]),
        ]
    )
    ket_far = jnp.stack(
        [
            jnp.concatenate([at_far + local_ket[2], at_far + inward[2]]),
            jnp.concatenate([local_ket[3], at_cross + capacity + spots]),
        ]
    )
    second = contract(bra_far, ket_far, [own, far, cross_far])

    kept_rows = bands // slices

    def part(array, side):
        return lax.dynamic_slice_in_dim(array, side * kept_rows, kept_rows, 1)

    def home(result, target):
        same = move(part(result, g), lambda p, s: (target(p), s))
        other = move(part(result, 1 - g), lambda p, s: (target(p), 1 - s))
        return same + other

    done_one = home(first[0], lambda p: p - PLANE if p % PLANE == PLANE - 1 else p)
    done_plane = home(first[1], lambda p: p - PLANE if p % 2 else p)
    done_far = jnp.where(stationary, part(second[0], g), 0.0)
    done_far = done_far + move(
        part(second[0], 1 - g), lambda p, s: None if moves_far(p) else (p, 1 - s)
    )
    done_far = done_far + move(
        part(second[1], g), lambda p, s: None if moves_far(p) else (p + half, s)
    )
    done_far = done_far + move(
        part(second[1], 1 - g), lambda p, s: None if moves_far(p) else (p + half, 1 - s)
    )
    done = jnp.stack([done_one, done_plane, done_far])
    chosen = is_aim[:, :, None, None, None]
    return jnp.sum(jnp.where(chosen, done[None], 0.0), axis=1)[None]


def solution(mesh):
    in_specs = (P("ka", "ga", None, None, None), P("ka", None), P("ka", None), P())
    out_specs = P("ka", None, None, "ga", None)
    return jax.shard_map(
        on_device, mesh=mesh, in_specs=in_specs, out_specs=out_specs, check_vma=False
    )
```

```python
import jax
import jax.numpy as jnp
from jax import lax
from jax.experimental import pallas as pl
from jax.experimental.pallas import tpu as pltpu
from jax.sharding import PartitionSpec as P

AXES = ("ka", "ga")
PLANE = 16
UNROLL = 12


def gather_kernel(counts, index_ref, source_ref, *refs):
    outs, (stage, sems) = refs[: len(counts)], refs[len(counts) :]
    total = sum(counts)

    def fetch(n, carry):
        pltpu.make_async_copy(source_ref.at[index_ref[n]], stage.at[n], sems.at[0]).start()
        return carry

    lax.fori_loop(0, total, fetch, 0)
    pltpu.make_async_copy(source_ref.at[pl.ds(0, total)], stage, sems.at[0]).wait()
    first = 0
    copies = []
    for slot, (out, count) in enumerate(zip(outs, counts)):
        copies.append(
            pltpu.make_async_copy(stage.at[pl.ds(first, count)], out, sems.at[slot + 1])
        )
        first += count
    for copy in copies:
        copy.start()
    for copy in copies:
        copy.wait()


def gather_blocks(source, index, counts):
    anywhere = pl.BlockSpec(memory_space=pl.ANY)
    return pl.pallas_call(
        lambda *refs: gather_kernel(counts, *refs),
        grid_spec=pltpu.PrefetchScalarGridSpec(
            num_scalar_prefetch=1,
            grid=(),
            in_specs=[anywhere],
            out_specs=[anywhere for _ in counts],
            scratch_shapes=[
                pltpu.VMEM((sum(counts),) + source.shape[1:], source.dtype),
                pltpu.SemaphoreType.DMA((len(counts) + 1,)),
            ],
        ),
        out_shape=[jax.ShapeDtypeStruct((n,) + source.shape[1:], source.dtype) for n in counts],
        name="gather_blocks",
    )(index, source)


def contract_kernel(sizes, tasks, terms, bra_ref, ket_ref, *refs):
    count = len(sizes)
    sources, out_ref, blocks, sems = refs[:count], refs[count], refs[count + 1], refs[count + 2]
    copies = []
    first = 0
    for slot, size in enumerate(sizes):
        copies.append(
            pltpu.make_async_copy(sources[slot], blocks.at[pl.ds(first, size)], sems.at[slot])
        )
        first += size
    for copy in copies:
        copy.start()
    for copy in copies:
        copy.wait()
    both = blocks.shape[1]
    bands = both // 2
    for task in range(tasks):

        def step(n, total, task=task):
            base = task * terms + n * UNROLL
            bra = jnp.concatenate([blocks[bra_ref[base + u]] for u in range(UNROLL)], axis=1)
            ket = jnp.concatenate([blocks[ket_ref[base + u]] for u in range(UNROLL)], axis=1)
            return total + lax.dot_general(
                bra, ket, (((1,), (1,)), ((), ())), preferred_element_type=jnp.float32
            )

        total = lax.fori_loop(0, terms // UNROLL, step, jnp.zeros((both, both), jnp.float32))
        out_ref[task, 0] = total[:bands, :bands] + total[bands:, bands:]
        out_ref[task, 1] = total[:bands, bands:] - total[bands:, :bands]


def contract(bra_index, ket_index, sources):
    tasks, terms = bra_index.shape
    sizes = [source.shape[0] for source in sources]
    block = sources[0].shape[1:]
    bands = block[0] // 2
    anywhere = pl.BlockSpec(memory_space=pl.ANY)
    return pl.pallas_call(
        lambda *refs: contract_kernel(sizes, tasks, terms, *refs),
        grid_spec=pltpu.PrefetchScalarGridSpec(
            num_scalar_prefetch=2,
            grid=(),
            in_specs=[anywhere for _ in sources],
            out_specs=pl.BlockSpec(memory_space=pltpu.VMEM),
            scratch_shapes=[
                pltpu.VMEM((sum(sizes),) + block, sources[0].dtype),
                pltpu.SemaphoreType.DMA((len(sizes),)),
            ],
        ),
        out_shape=jax.ShapeDtypeStruct((tasks, 2, bands, bands), jnp.float32),
        name="contract",
    )(bra_index.reshape(-1), ket_index.reshape(-1), *sources)


def compact(flag, value, count):
    size = flag.shape[1]
    earlier = jnp.arange(size)[:, None] < jnp.arange(size)[None, :]
    rank = jnp.sum(flag[:, :, None] & earlier[None], axis=1, dtype=jnp.int32)
    hit = flag[:, None, :] & (rank[:, None, :] == jnp.arange(count)[None, :, None])
    return jnp.sum(jnp.where(hit, value[:, None, :], 0), axis=2, dtype=jnp.int32)


def on_device(coeffs, neighbour, shift_id, block_map):
    slab = coeffs.shape[1]
    bands, lanes = coeffs.shape[3], coeffs.shape[4]
    points, slices = lax.axis_size("ka"), lax.axis_size("ga")
    capacity = slab // 6
    k = lax.axis_index("ka")
    g = lax.axis_index("ga")
    plane_place = k % PLANE
    last = plane_place == PLANE - 1
    upward = k % 2 == 1
    stationary = (k < points // 2) == upward
    half = points // 2

    def route(target):
        pairs = []
        for point in range(points):
            for side in range(slices):
                to = target(point, side)
                if to is not None:
                    pairs.append((point * slices + side, to[0] % points * slices + to[1]))
        return pairs

    def move(array, target):
        return lax.ppermute(array, AXES, route(target))

    def moves_far(point):
        return (point < half) == (point % 2 == 0)

    own = coeffs.reshape(slab, 2 * bands, lanes)
    near = move(own, lambda p, s: (p + PLANE if p % 2 else p - PLANE, s))
    far = move(own, lambda p, s: (p + half, s) if moves_far(p) else None)
    ring = move(own, lambda p, s: (p // PLANE * PLANE + (p - 1) % PLANE, s))

    aims = jnp.stack([(k + step) % points for step in (1, PLANE, half)])
    is_aim = neighbour[0][:, None] == aims[None, :]
    shifts = jnp.sum(jnp.where(is_aim, shift_id[0][:, None], 0), axis=0, dtype=jnp.int32)
    shifts_below = move(shifts, lambda p, s: (p + PLANE, s))
    shifts_before = move(shifts, lambda p, s: (p + 1, s))
    shifts_far = move(shifts, lambda p, s: (p + half, s))
    rows = jnp.stack(
        [
            jnp.where(last, shifts_below[0], shifts[0]),
            jnp.where(upward, shifts_below[1], shifts[1]),
            shifts[2],
            shifts_far[2],
            shifts_before[0],
        ]
    )
    picked = rows[:, None] == jnp.arange(block_map.shape[0])[None, :]
    relabel = jnp.sum(jnp.where(picked[:, :, None], block_map[None], 0), axis=1, dtype=jnp.int32)
    dest = jnp.broadcast_to(jnp.arange(relabel.shape[1], dtype=jnp.int32), relabel.shape)
    here, there = dest // slab == g, relabel // slab == g
    dest_local, source_local = dest - g * slab, relabel - g * slab
    outward = compact(here & ~there, dest_local, capacity)
    inward = compact(~here & there, source_local, capacity)
    local_bra = compact(here & there, dest_local, slab - capacity)
    local_ket = compact(here & there, source_local, slab - capacity)

    payload = jnp.concatenate(
        [
            outward[0],
            jnp.where(upward, inward[1], outward[1]),
            outward[2],
            inward[3],
            inward[4],
        ]
    )
    pay_one, pay_plane, pay_far, pay_wrap = gather_blocks(
        own, payload, (capacity, capacity, 2 * capacity, capacity)
    )
    cross_one = move(pay_one, lambda p, s: (p, 1 - s) if p % PLANE != PLANE - 1 else None)
    cross_plane = move(pay_plane, lambda p, s: (p, 1 - s))
    cross_far = move(pay_far, lambda p, s: None if moves_far(p) else (p, 1 - s))
    cross_wrap = move(
        pay_wrap, lambda p, s: (p + PLANE - 1, 1 - s) if p % PLANE == 0 else None
    )

    spots = jnp.arange(capacity, dtype=jnp.int32)
    at_near, at_ring, at_one = slab, 2 * slab, 3 * slab
    at_wrap, at_plane = at_one + capacity, at_one + 2 * capacity
    bra_one = jnp.concatenate(
        [
            local_bra[0] + jnp.where(last, at_near, 0),
            jnp.where(last, at_near + outward[0], at_one + spots),
        ]
    )
    ket_one = jnp.concatenate(
        [at_ring + local_ket[0], jnp.where(last, at_wrap + spots, at_ring + inward[0])]
    )
    bra_plane = jnp.concatenate(
        [
            local_bra[1] + jnp.where(upward, at_near, 0),
            jnp.where(upward, at_near + outward[1], at_plane + spots),
        ]
    )
    ket_plane = jnp.concatenate(
        [
            local_ket[1] + jnp.where(upward, 0, at_near),
            jnp.where(upward, at_plane + spots, at_near + inward[1]),
        ]
    )
    first = contract(
        jnp.stack([bra_one, bra_plane]),
        jnp.stack([ket_one, ket_plane]),
        [own, near, ring, cross_one, cross_wrap, cross_plane],
    )
    at_far, at_cross = slab, 2 * slab
    bra_far = jnp.stack(
        [
            jnp.concatenate([local_bra[2], at_cross + spots]),
            jnp.concatenate([at_far + local_bra[3], at_far + outward[3]]),
        ]
    )
    ket_far = jnp.stack(
        [
            jnp.concatenate([at_far + local_ket[2], at_far + inward[2]]),
            jnp.concatenate([local_ket[3], at_cross + capacity + spots]),
        ]
    )
    second = contract(bra_far, ket_far, [own, far, cross_far])

    kept_rows = bands // slices

    def part(array, side):
        return lax.dynamic_slice_in_dim(array, side * kept_rows, kept_rows, 1)

    def home(result, target):
        same = move(part(result, g), lambda p, s: (target(p), s))
        other = move(part(result, 1 - g), lambda p, s: (target(p), 1 - s))
        return same + other

    done_one = home(first[0], lambda p: p - PLANE if p % PLANE == PLANE - 1 else p)
    done_plane = home(first[1], lambda p: p - PLANE if p % 2 else p)
    done_far = jnp.where(stationary, part(second[0], g), 0.0)
    done_far = done_far + move(
        part(second[0], 1 - g), lambda p, s: None if moves_far(p) else (p, 1 - s)
    )
    done_far = done_far + move(
        part(second[1], g), lambda p, s: None if moves_far(p) else (p + half, s)
    )
    done_far = done_far + move(
        part(second[1], 1 - g), lambda p, s: None if moves_far(p) else (p + half, 1 - s)
    )
    done = jnp.stack([done_one, done_plane, done_far])
    chosen = is_aim[:, :, None, None, None]
    return jnp.sum(jnp.where(chosen, done[None], 0.0), axis=1)[None]


def solution(mesh):
    in_specs = (P("ka", "ga", None, None, None), P("ka", None), P("ka", None), P())
    out_specs = P("ka", None, None, "ga", None)
    return jax.shard_map(
        on_device, mesh=mesh, in_specs=in_specs, out_specs=out_specs, check_vma=False
    )
```

```python
import jax
import jax.numpy as jnp
from jax import lax
from jax.experimental import pallas as pl
from jax.experimental.pallas import tpu as pltpu
from jax.sharding import PartitionSpec as P


AXES = ("ka", "ga")
PLANE = 16
UNROLL = 12
CHUNKS = (48, 48, 24)
PAIR_UNROLL = 8


def gather_kernel(counts, index_ref, source_ref, *refs):
    outs, (stage, sems) = refs[: len(counts)], refs[len(counts) :]
    total = sum(counts)

    def fetch(n, carry):
        pltpu.make_async_copy(source_ref.at[index_ref[n]], stage.at[n], sems.at[0]).start()
        return carry

    lax.fori_loop(0, total, fetch, 0)
    pltpu.make_async_copy(source_ref.at[pl.ds(0, total)], stage, sems.at[0]).wait()
    first = 0
    copies = []
    for slot, (out, count) in enumerate(zip(outs, counts)):
        copies.append(
            pltpu.make_async_copy(stage.at[pl.ds(first, count)], out, sems.at[slot + 1])
        )
        first += count
    for copy in copies:
        copy.start()
    for copy in copies:
        copy.wait()


def gather_blocks(source, index, counts):
    anywhere = pl.BlockSpec(memory_space=pl.ANY)
    return pl.pallas_call(
        lambda *refs: gather_kernel(counts, *refs),
        grid_spec=pltpu.PrefetchScalarGridSpec(
            num_scalar_prefetch=1,
            grid=(),
            in_specs=[anywhere],
            out_specs=[anywhere for _ in counts],
            scratch_shapes=[
                pltpu.VMEM((sum(counts),) + source.shape[1:], source.dtype),
                pltpu.SemaphoreType.DMA((len(counts) + 1,)),
            ],
        ),
        out_shape=[jax.ShapeDtypeStruct((n,) + source.shape[1:], source.dtype) for n in counts],
        name="gather_blocks",
    )(index, source)


def contract_kernel(sizes, tasks, terms, bra_ref, ket_ref, active_ref, use_ref, *refs):
    sources, (blocks, sems) = refs[: len(sizes)], refs[-2:]
    outs = refs[-2 - tasks : -2]

    def staged(act):
        first = 0
        for slot, size in enumerate(sizes):

            @pl.when(use_ref[slot] > 0)
            def _(slot=slot, size=size, first=first):
                act(
                    pltpu.make_async_copy(
                        sources[slot], blocks.at[pl.ds(first, size)], sems.at[slot]
                    )
                )

            first += size

    staged(lambda copy: copy.start())
    staged(lambda copy: copy.wait())
    both = blocks.shape[1]
    bands = both // 2
    for task in range(tasks):

        def step(n, total, task=task):
            base = task * terms + n * UNROLL
            bra = jnp.concatenate([blocks[bra_ref[base + u]] for u in range(UNROLL)], axis=1)
            ket = jnp.concatenate([blocks[ket_ref[base + u]] for u in range(UNROLL)], axis=1)
            return total + lax.dot_general(
                bra, ket, (((1,), (1,)), ((), ())), preferred_element_type=jnp.float32
            )

        steps = jnp.where(active_ref[task] > 0, terms // UNROLL, 0)
        total = lax.fori_loop(0, steps, step, jnp.zeros((both, both), jnp.float32))
        outs[task][0] = total[:bands, :bands] + total[bands:, bands:]
        outs[task][1] = total[:bands, bands:] - total[bands:, :bands]


def contract(bra_index, ket_index, active, sources, use=None, after=()):
    tasks, terms = bra_index.shape
    use = active * len(sources) if use is None else use
    sizes = [source.shape[0] for source in sources]
    block = sources[0].shape[1:]
    bands = block[0] // 2
    anywhere = pl.BlockSpec(memory_space=pl.ANY)
    return pl.pallas_call(
        lambda *refs: contract_kernel(sizes, tasks, terms, *refs),
        grid_spec=pltpu.PrefetchScalarGridSpec(
            num_scalar_prefetch=4,
            grid=(),
            in_specs=[anywhere for _ in (*sources, *after)],
            out_specs=[pl.BlockSpec(memory_space=pltpu.VMEM)] * tasks,
            scratch_shapes=[
                pltpu.VMEM((sum(sizes),) + block, sources[0].dtype),
                pltpu.SemaphoreType.DMA((len(sizes),)),
            ],
        ),
        out_shape=[jax.ShapeDtypeStruct((2, bands, bands), jnp.float32)] * tasks,
        name="contract",
    )(
        bra_index.reshape(-1),
        ket_index.reshape(-1),
        jnp.stack(active).astype(jnp.int32),
        jnp.stack(use).astype(jnp.int32),
        *sources,
        *after,
    )


def split_kernel(source_ref, *refs):
    outs, (stage, sems) = refs[:-2], refs[-2:]
    copies, first = [], 0
    for slot, out in enumerate(outs):
        piece = stage.at[pl.ds(first, out.shape[0])]
        copies.append(
            (
                pltpu.make_async_copy(
                    source_ref.at[pl.ds(first, out.shape[0])], piece, sems.at[0, slot]
                ),
                pltpu.make_async_copy(piece, out, sems.at[1, slot]),
            )
        )
        first += out.shape[0]
    for fetch, _ in copies:
        fetch.start()
    for fetch, store in copies:
        fetch.wait()
        store.start()
    for _, store in copies:
        store.wait()


def split_blocks(source, sizes):
    anywhere = pl.BlockSpec(memory_space=pl.ANY)
    block, parts = source.shape[1:], len(sizes)
    return pl.pallas_call(
        split_kernel,
        in_specs=[anywhere],
        out_specs=[anywhere for _ in range(parts)],
        scratch_shapes=[
            pltpu.VMEM(source.shape, source.dtype),
            pltpu.SemaphoreType.DMA((2, parts)),
        ],
        out_shape=[jax.ShapeDtypeStruct((size,) + block, source.dtype) for size in sizes],
        name="split_blocks",
    )(source)


def pair_kernel(sizes, index_ref, active_ref, moved_ref, *refs):
    count = len(sizes)
    sources = refs[:count]
    start_ref, out_ref, moved, blocks, sems = refs[count], *refs[-4:]
    out_ref[...] = start_ref[...]

    @pl.when(active_ref[0] > 0)
    def _():
        copies = [pltpu.make_async_copy(moved_ref, moved, sems.at[count])]
        first = 0
        for slot, size in enumerate(sizes):
            copies.append(
                pltpu.make_async_copy(
                    sources[slot], blocks.at[pl.ds(first, size)], sems.at[slot]
                )
            )
            first += size
        for copy in copies:
            copy.start()
        for copy in copies:
            copy.wait()
        terms = moved.shape[0]

        def step(n, total):
            base = n * PAIR_UNROLL
            left = [
                jnp.concatenate(
                    [blocks[index_ref[side * terms + base + u]] for u in range(PAIR_UNROLL)],
                    axis=1,
                )
                for side in range(2)
            ]
            right = jnp.concatenate([moved[base + u] for u in range(PAIR_UNROLL)], axis=1)
            return total + lax.dot_general(
                jnp.concatenate(left, axis=0),
                right,
                (((1,), (1,)), ((), ())),
                preferred_element_type=jnp.float32,
            )

        out_ref[...] = lax.fori_loop(0, terms // PAIR_UNROLL, step, out_ref[...])


def contract_pair(index, active, moved, sources, start, after=()):
    sizes = [source.shape[0] for source in sources]
    anywhere = pl.BlockSpec(memory_space=pl.ANY)
    local = pl.BlockSpec(memory_space=pltpu.VMEM)
    return pl.pallas_call(
        lambda *refs: pair_kernel(sizes, *refs),
        grid_spec=pltpu.PrefetchScalarGridSpec(
            num_scalar_prefetch=2,
            grid=(),
            in_specs=[anywhere] + [anywhere for _ in sources] + [local] + [anywhere for _ in after],
            out_specs=local,
            scratch_shapes=[
                pltpu.VMEM(moved.shape, moved.dtype),
                pltpu.VMEM((sum(sizes),) + moved.shape[1:], moved.dtype),
                pltpu.SemaphoreType.DMA((len(sizes) + 1,)),
            ],
        ),
        out_shape=jax.ShapeDtypeStruct(start.shape, jnp.float32),
        name="contract_pair",
    )(index.reshape(-1), active.astype(jnp.int32)[None], moved, *sources, start, *after)


def products(total):
    bands = total.shape[1] // 2
    first, second = total[: 2 * bands], total[2 * bands :]
    one = jnp.stack(
        [
            first[:bands, :bands] + first[bands:, bands:],
            first[:bands, bands:] - first[bands:, :bands],
        ]
    )
    other = jnp.stack(
        [
            (second[:bands, :bands] + second[bands:, bands:]).T,
            (second[bands:, :bands] - second[:bands, bands:]).T,
        ]
    )
    return one, other


def ranks(flag):
    size = flag.shape[1]
    earlier = jnp.arange(size)[:, None] < jnp.arange(size)[None, :]
    return jnp.sum(flag[:, :, None] & earlier[None], axis=1, dtype=jnp.int32)


def compact(flag, value, count):
    rank = ranks(flag)
    hit = flag[:, None, :] & (rank[:, None, :] == jnp.arange(count)[None, :, None])
    return jnp.sum(jnp.where(hit, value[:, None, :], 0), axis=2, dtype=jnp.int32)


def step(coeffs, neighbour, shift_id, block_map):
    slab = coeffs.shape[1]
    bands, lanes = coeffs.shape[3], coeffs.shape[4]
    points, slices = lax.axis_size("ka"), lax.axis_size("ga")
    capacity = slab // 6
    k = lax.axis_index("ka")
    g = lax.axis_index("ga")
    plane_place = k % PLANE
    last = plane_place == PLANE - 1
    upward = k % 2 == 1
    stationary = (k < points // 2) == upward
    half = points // 2

    def route(target):
        pairs = []
        for point in range(points):
            for side in range(slices):
                to = target(point, side)
                if to is not None:
                    pairs.append((point * slices + side, to[0] % points * slices + to[1]))
        return pairs

    def move(array, target):
        return lax.ppermute(array, AXES, route(target))

    def moves_far(point):
        return (point < half) == (point % 2 == 0)

    own = coeffs.reshape(slab, 2 * bands, lanes)
    near = move(own, lambda p, s: (p + PLANE if p % 2 else p - PLANE, s))
    far = [
        move(piece, lambda p, s: (p + half, s) if moves_far(p) else None)
        for piece in split_blocks(own, CHUNKS)
    ]
    ring = move(own, lambda p, s: (p // PLANE * PLANE + (p - 1) % PLANE, s))

    aims = jnp.stack([(k + step) % points for step in (1, PLANE, half)])
    is_aim = neighbour[0][:, None] == aims[None, :]
    shifts = jnp.sum(jnp.where(is_aim, shift_id[0][:, None], 0), axis=0, dtype=jnp.int32)
    shifts_below = move(shifts, lambda p, s: (p + PLANE, s))
    shifts_before = move(shifts, lambda p, s: (p + 1, s))
    shifts_far = move(shifts, lambda p, s: (p + half, s))
    rows = jnp.stack(
        [
            jnp.where(last, shifts_below[0], shifts[0]),
            jnp.where(upward, shifts_below[1], shifts[1]),
            shifts[2],
            shifts_far[2],
            shifts_before[0],
        ]
    )
    picked = rows[:, None] == jnp.arange(block_map.shape[0])[None, :]
    relabel = jnp.sum(jnp.where(picked[:, :, None], block_map[None], 0), axis=1, dtype=jnp.int32)
    dest = jnp.broadcast_to(jnp.arange(relabel.shape[1], dtype=jnp.int32), relabel.shape)
    here, there = dest // slab == g, relabel // slab == g
    dest_local, source_local = dest - g * slab, relabel - g * slab
    outward = compact(here & ~there, dest_local, capacity)
    inward = compact(~here & there, source_local, capacity)
    local_bra = compact(here & there, dest_local, slab - capacity)
    local_ket = compact(here & there, source_local, slab - capacity)

    payload = jnp.concatenate(
        [
            outward[0],
            jnp.where(upward, inward[1], outward[1]),
            outward[2],
            inward[3],
            inward[4],
        ]
    )
    pay_one, pay_plane, pay_far, pay_wrap = gather_blocks(
        own, payload, (capacity, capacity, 2 * capacity, capacity)
    )
    cross_one = move(pay_one, lambda p, s: (p, 1 - s) if p % PLANE != PLANE - 1 else None)
    cross_plane = move(pay_plane, lambda p, s: (p, 1 - s))
    cross_far = move(pay_far, lambda p, s: None if moves_far(p) else (p, 1 - s))
    cross_wrap = move(
        pay_wrap, lambda p, s: (p + PLANE - 1, 1 - s) if p % PLANE == 0 else None
    )

    spots_all = jnp.arange(slab, dtype=jnp.int32)
    spots = spots_all[:capacity]
    at_plane, at_cross = slab, 2 * slab
    bra_plane = jnp.concatenate(
        [
            local_bra[1] + jnp.where(upward, at_plane, 0),
            jnp.where(upward, at_plane + outward[1], at_cross + spots),
        ]
    )
    ket_plane = jnp.concatenate(
        [
            local_ket[1] + jnp.where(upward, 0, at_plane),
            jnp.where(upward, at_cross + spots, at_plane + inward[1]),
        ]
    )
    one_early = contract(
        jnp.concatenate([local_bra[0], 2 * slab + spots])[None],
        jnp.concatenate([slab + local_ket[0], slab + inward[0]])[None],
        [~last],
        [own, ring, cross_one],
    )[0]
    here, there = here[2:4], there[2:4]
    leaving_rank = ranks(here & ~there)[1]
    coming_rank = ranks(~here & there)[0]
    with_ket = jnp.where(here[0], dest_local[2], slab + coming_rank)
    mine = g * slab + spots_all
    hit = relabel[2][None, :] == mine[:, None]
    first_partner = jnp.sum(jnp.where(hit, with_ket[None], 0), axis=1, dtype=jnp.int32)
    second_partner = lax.dynamic_slice_in_dim(
        jnp.where(there[1], source_local[3], slab + capacity + leaving_rank), g * slab, slab
    )
    at_ring, at_wrap = 2 * slab + capacity, 3 * slab + capacity
    bra_near = [bra_plane, jnp.concatenate([at_plane + local_bra[0], at_plane + outward[0]])]
    ket_near = [ket_plane, jnp.concatenate([at_ring + local_ket[0], at_wrap + spots])]
    total = jnp.zeros((4 * bands, 2 * bands), jnp.float32)
    first = 0
    after = (one_early,)
    for n, piece in enumerate(far):
        index = jnp.stack([x[first : first + piece.shape[0]] for x in (first_partner, second_partner)])
        first += piece.shape[0]
        total = contract_pair(index, stationary, piece, [own, cross_far], total, after)
        after = ()
        if n == len(far) - 2:
            plane_sum, one_late = contract(
                jnp.stack(bra_near),
                jnp.stack(ket_near),
                [True | last, last],
                [own, near, cross_plane, ring, cross_wrap],
                [True | last] * 3 + [last] * 2,
                after=(total,),
            )
            after = (plane_sum,)
    far_first, far_second = products(total)
    sent_far = move(
        far_second, lambda p, s: None if moves_far(p) else (p + half, s)
    )
    sent_down = move(
        jnp.stack([plane_sum, one_late]), lambda p, s: (p - PLANE, s) if p % 2 else None
    )
    totals = jnp.stack(
        [
            jnp.where(last, sent_down[1], one_early),
            jnp.where(upward, sent_down[0], plane_sum),
            jnp.where(stationary, far_first, sent_far),
        ]
    )
    kept_rows = bands // slices

    def part(side):
        return lax.dynamic_slice_in_dim(totals, side * kept_rows, kept_rows, 2)

    done = part(g) + move(part(1 - g), lambda p, s: (p, 1 - s))
    chosen = is_aim[:, :, None, None, None]
    return jnp.sum(jnp.where(chosen, done[None], 0.0), axis=1)[None]


def solution(mesh):
    in_specs = (P("ka", "ga", None, None, None), P("ka", None), P("ka", None), P())
    out_specs = P("ka", None, None, "ga", None)
    return jax.shard_map(step, mesh=mesh, in_specs=in_specs, out_specs=out_specs, check_vma=False)
```

```python
import jax
import jax.numpy as jnp
from jax import lax
from jax.experimental import pallas as pl
from jax.experimental.pallas import tpu as pltpu
from jax.sharding import PartitionSpec as P


AXES = ("ka", "ga")
PLANE = 16
UNROLL = 24
CHUNKS = (72, 48)
PAIR_UNROLL = 24


def gather_kernel(counts, index_ref, source_ref, *refs):
    outs, (stage, sems) = refs[: len(counts)], refs[len(counts) :]
    total = sum(counts)

    def fetch(n, carry):
        pltpu.make_async_copy(source_ref.at[index_ref[n]], stage.at[n], sems.at[0]).start()
        return carry

    lax.fori_loop(0, total, fetch, 0)
    pltpu.make_async_copy(source_ref.at[pl.ds(0, total)], stage, sems.at[0]).wait()
    first = 0
    copies = []
    for slot, (out, count) in enumerate(zip(outs, counts)):
        copies.append(
            pltpu.make_async_copy(stage.at[pl.ds(first, count)], out, sems.at[slot + 1])
        )
        first += count
    for copy in copies:
        copy.start()
    for copy in copies:
        copy.wait()


def gather_blocks(source, index, counts):
    anywhere = pl.BlockSpec(memory_space=pl.ANY)
    return pl.pallas_call(
        lambda *refs: gather_kernel(counts, *refs),
        grid_spec=pltpu.PrefetchScalarGridSpec(
            num_scalar_prefetch=1,
            grid=(),
            in_specs=[anywhere],
            out_specs=[anywhere for _ in counts],
            scratch_shapes=[
                pltpu.VMEM((sum(counts),) + source.shape[1:], source.dtype),
                pltpu.SemaphoreType.DMA((len(counts) + 1,)),
            ],
        ),
        out_shape=[jax.ShapeDtypeStruct((n,) + source.shape[1:], source.dtype) for n in counts],
        name="gather_blocks",
    )(index, source)


def contract_kernel(sizes, tasks, terms, bra_ref, ket_ref, active_ref, use_ref, *refs):
    sources, (blocks, sems) = refs[: len(sizes)], refs[-2:]
    outs = refs[-2 - tasks : -2]

    def staged(act):
        first = 0
        for slot, size in enumerate(sizes):

            @pl.when(use_ref[slot] > 0)
            def _(slot=slot, size=size, first=first):
                act(
                    pltpu.make_async_copy(
                        sources[slot], blocks.at[pl.ds(first, size)], sems.at[slot]
                    )
                )

            first += size

    staged(lambda copy: copy.start())
    staged(lambda copy: copy.wait())
    both = blocks.shape[1]
    bands = both // 2
    for task in range(tasks):

        def step(n, total, task=task):
            base = task * terms + n * UNROLL
            bra = jnp.concatenate([blocks[bra_ref[base + u]] for u in range(UNROLL)], axis=1)
            ket = jnp.concatenate([blocks[ket_ref[base + u]] for u in range(UNROLL)], axis=1)
            return total + lax.dot_general(
                bra, ket, (((1,), (1,)), ((), ())), preferred_element_type=jnp.float32
            )

        steps = jnp.where(active_ref[task] > 0, terms // UNROLL, 0)
        total = lax.fori_loop(0, steps, step, jnp.zeros((both, both), jnp.float32))
        outs[task][0] = total[:bands, :bands] + total[bands:, bands:]
        outs[task][1] = total[:bands, bands:] - total[bands:, :bands]


def contract(bra_index, ket_index, active, sources, use=None, after=()):
    tasks, terms = bra_index.shape
    use = active * len(sources) if use is None else use
    sizes = [source.shape[0] for source in sources]
    block = sources[0].shape[1:]
    bands = block[0] // 2
    anywhere = pl.BlockSpec(memory_space=pl.ANY)
    return pl.pallas_call(
        lambda *refs: contract_kernel(sizes, tasks, terms, *refs),
        grid_spec=pltpu.PrefetchScalarGridSpec(
            num_scalar_prefetch=4,
            grid=(),
            in_specs=[anywhere for _ in (*sources, *after)],
            out_specs=[pl.BlockSpec(memory_space=pltpu.VMEM)] * tasks,
            scratch_shapes=[
                pltpu.VMEM((sum(sizes),) + block, sources[0].dtype),
                pltpu.SemaphoreType.DMA((len(sizes),)),
            ],
        ),
        out_shape=[jax.ShapeDtypeStruct((2, bands, bands), jnp.float32)] * tasks,
        name="contract",
    )(
        bra_index.reshape(-1),
        ket_index.reshape(-1),
        jnp.stack(active).astype(jnp.int32),
        jnp.stack(use).astype(jnp.int32),
        *sources,
        *after,
    )


def split_kernel(source_ref, *refs):
    outs, (stage, sems) = refs[:-2], refs[-2:]
    copies, first = [], 0
    for slot, out in enumerate(outs):
        piece = stage.at[pl.ds(first, out.shape[0])]
        copies.append(
            (
                pltpu.make_async_copy(
                    source_ref.at[pl.ds(first, out.shape[0])], piece, sems.at[0, slot]
                ),
                pltpu.make_async_copy(piece, out, sems.at[1, slot]),
            )
        )
        first += out.shape[0]
    for fetch, _ in copies:
        fetch.start()
    for fetch, store in copies:
        fetch.wait()
        store.start()
    for _, store in copies:
        store.wait()


def split_blocks(source, sizes):
    anywhere = pl.BlockSpec(memory_space=pl.ANY)
    block, parts = source.shape[1:], len(sizes)
    return pl.pallas_call(
        split_kernel,
        in_specs=[anywhere],
        out_specs=[anywhere for _ in range(parts)],
        scratch_shapes=[
            pltpu.VMEM(source.shape, source.dtype),
            pltpu.SemaphoreType.DMA((2, parts)),
        ],
        out_shape=[jax.ShapeDtypeStruct((size,) + block, source.dtype) for size in sizes],
        name="split_blocks",
    )(source)


def pair_kernel(sizes, index_ref, active_ref, moved_ref, *refs):
    count = len(sizes)
    sources = refs[:count]
    start_ref, out_ref, moved, blocks, sems = refs[count], *refs[-4:]
    out_ref[...] = start_ref[...]

    @pl.when(active_ref[0] > 0)
    def _():
        copies = [pltpu.make_async_copy(moved_ref, moved, sems.at[count])]
        first = 0
        for slot, size in enumerate(sizes):
            copies.append(
                pltpu.make_async_copy(
                    sources[slot], blocks.at[pl.ds(first, size)], sems.at[slot]
                )
            )
            first += size
        for copy in copies:
            copy.start()
        for copy in copies:
            copy.wait()
        terms = moved.shape[0]

        def step(n, total):
            base = n * PAIR_UNROLL
            left = [
                jnp.concatenate(
                    [blocks[index_ref[side * terms + base + u]] for u in range(PAIR_UNROLL)],
                    axis=1,
                )
                for side in range(2)
            ]
            right = jnp.concatenate([moved[base + u] for u in range(PAIR_UNROLL)], axis=1)
            return total + lax.dot_general(
                jnp.concatenate(left, axis=0),
                right,
                (((1,), (1,)), ((), ())),
                preferred_element_type=jnp.float32,
            )

        out_ref[...] = lax.fori_loop(0, terms // PAIR_UNROLL, step, out_ref[...])


def contract_pair(index, active, moved, sources, start, after=()):
    sizes = [source.shape[0] for source in sources]
    anywhere = pl.BlockSpec(memory_space=pl.ANY)
    local = pl.BlockSpec(memory_space=pltpu.VMEM)
    return pl.pallas_call(
        lambda *refs: pair_kernel(sizes, *refs),
        grid_spec=pltpu.PrefetchScalarGridSpec(
            num_scalar_prefetch=2,
            grid=(),
            in_specs=[anywhere] + [anywhere for _ in sources] + [local] + [anywhere for _ in after],
            out_specs=local,
            scratch_shapes=[
                pltpu.VMEM(moved.shape, moved.dtype),
                pltpu.VMEM((sum(sizes),) + moved.shape[1:], moved.dtype),
                pltpu.SemaphoreType.DMA((len(sizes) + 1,)),
            ],
        ),
        out_shape=jax.ShapeDtypeStruct(start.shape, jnp.float32),
        name="contract_pair",
    )(index.reshape(-1), active.astype(jnp.int32)[None], moved, *sources, start, *after)


def products(total):
    bands = total.shape[1] // 2
    first, second = total[: 2 * bands], total[2 * bands :]
    one = jnp.stack(
        [
            first[:bands, :bands] + first[bands:, bands:],
            first[:bands, bands:] - first[bands:, :bands],
        ]
    )
    other = jnp.stack(
        [
            (second[:bands, :bands] + second[bands:, bands:]).T,
            (second[bands:, :bands] - second[:bands, bands:]).T,
        ]
    )
    return one, other


def ranks(flag):
    size = flag.shape[1]
    earlier = jnp.arange(size)[:, None] < jnp.arange(size)[None, :]
    return jnp.sum(flag[:, :, None] & earlier[None], axis=1, dtype=jnp.int32)


def compact(flag, value, count):
    rank = ranks(flag)
    hit = flag[:, None, :] & (rank[:, None, :] == jnp.arange(count)[None, :, None])
    return jnp.sum(jnp.where(hit, value[:, None, :], 0), axis=2, dtype=jnp.int32)


def step(coeffs, neighbour, shift_id, block_map):
    slab = coeffs.shape[1]
    bands, lanes = coeffs.shape[3], coeffs.shape[4]
    points, slices = lax.axis_size("ka"), lax.axis_size("ga")
    capacity = slab // 6
    k = lax.axis_index("ka")
    g = lax.axis_index("ga")
    plane_place = k % PLANE
    last = plane_place == PLANE - 1
    upward = k % 2 == 1
    stationary = (k < points // 2) == upward
    half = points // 2

    def route(target):
        pairs = []
        for point in range(points):
            for side in range(slices):
                to = target(point, side)
                if to is not None:
                    pairs.append((point * slices + side, to[0] % points * slices + to[1]))
        return pairs

    def move(array, target):
        return lax.ppermute(array, AXES, route(target))

    def moves_far(point):
        return (point < half) == (point % 2 == 0)

    own = coeffs.reshape(slab, 2 * bands, lanes)
    near = move(own, lambda p, s: (p + PLANE if p % 2 else p - PLANE, s))
    far = [
        move(piece, lambda p, s: (p + half, s) if moves_far(p) else None)
        for piece in split_blocks(own, CHUNKS)
    ]
    ring = move(own, lambda p, s: (p // PLANE * PLANE + (p - 1) % PLANE, s))

    aims = jnp.stack([(k + step) % points for step in (1, PLANE, half)])
    is_aim = neighbour[0][:, None] == aims[None, :]
    shifts = jnp.sum(jnp.where(is_aim, shift_id[0][:, None], 0), axis=0, dtype=jnp.int32)
    shifts_below = move(shifts, lambda p, s: (p + PLANE, s))
    shifts_before = move(shifts, lambda p, s: (p + 1, s))
    shifts_far = move(shifts, lambda p, s: (p + half, s))
    rows = jnp.stack(
        [
            jnp.where(last, shifts_below[0], shifts[0]),
            jnp.where(upward, shifts_below[1], shifts[1]),
            shifts[2],
            shifts_far[2],
            shifts_before[0],
        ]
    )
    picked = rows[:, None] == jnp.arange(block_map.shape[0])[None, :]
    relabel = jnp.sum(jnp.where(picked[:, :, None], block_map[None], 0), axis=1, dtype=jnp.int32)
    dest = jnp.broadcast_to(jnp.arange(relabel.shape[1], dtype=jnp.int32), relabel.shape)
    here, there = dest // slab == g, relabel // slab == g
    dest_local, source_local = dest - g * slab, relabel - g * slab
    outward = compact(here & ~there, dest_local, capacity)
    inward = compact(~here & there, source_local, capacity)
    local_bra = compact(here & there, dest_local, slab - capacity)
    local_ket = compact(here & there, source_local, slab - capacity)

    payload = jnp.concatenate(
        [
            outward[0],
            jnp.where(upward, inward[1], outward[1]),
            outward[2],
            inward[3],
            inward[4],
        ]
    )
    pay_one, pay_plane, pay_far, pay_wrap = gather_blocks(
        own, payload, (capacity, capacity, 2 * capacity, capacity)
    )
    cross_one = move(pay_one, lambda p, s: (p, 1 - s) if p % PLANE != PLANE - 1 else None)
    cross_plane = move(pay_plane, lambda p, s: (p, 1 - s))
    cross_far = move(pay_far, lambda p, s: None if moves_far(p) else (p, 1 - s))
    cross_wrap = move(
        pay_wrap, lambda p, s: (p + PLANE - 1, 1 - s) if p % PLANE == 0 else None
    )

    spots_all = jnp.arange(slab, dtype=jnp.int32)
    spots = spots_all[:capacity]
    at_plane, at_cross = slab, 2 * slab
    bra_plane = jnp.concatenate(
        [
            local_bra[1] + jnp.where(upward, at_plane, 0),
            jnp.where(upward, at_plane + outward[1], at_cross + spots),
        ]
    )
    ket_plane = jnp.concatenate(
        [
            local_ket[1] + jnp.where(upward, 0, at_plane),
            jnp.where(upward, at_cross + spots, at_plane + inward[1]),
        ]
    )
    one_early = contract(
        jnp.concatenate([local_bra[0], 2 * slab + spots])[None],
        jnp.concatenate([slab + local_ket[0], slab + inward[0]])[None],
        [~last],
        [own, ring, cross_one],
    )[0]
    here, there = here[2:4], there[2:4]
    leaving_rank = ranks(here & ~there)[1]
    coming_rank = ranks(~here & there)[0]
    with_ket = jnp.where(here[0], dest_local[2], slab + coming_rank)
    mine = g * slab + spots_all
    hit = relabel[2][None, :] == mine[:, None]
    first_partner = jnp.sum(jnp.where(hit, with_ket[None], 0), axis=1, dtype=jnp.int32)
    second_partner = lax.dynamic_slice_in_dim(
        jnp.where(there[1], source_local[3], slab + capacity + leaving_rank), g * slab, slab
    )
    at_ring, at_wrap = 2 * slab + capacity, 3 * slab + capacity
    bra_near = [bra_plane, jnp.concatenate([at_plane + local_bra[0], at_plane + outward[0]])]
    ket_near = [ket_plane, jnp.concatenate([at_ring + local_ket[0], at_wrap + spots])]
    total = jnp.zeros((4 * bands, 2 * bands), jnp.float32)
    first = 0
    after = (one_early,)
    for n, piece in enumerate(far):
        index = jnp.stack([x[first : first + piece.shape[0]] for x in (first_partner, second_partner)])
        first += piece.shape[0]
        total = contract_pair(index, stationary, piece, [own, cross_far], total, after)
        after = ()
        if n == len(far) - 2:
            plane_sum, one_late = contract(
                jnp.stack(bra_near),
                jnp.stack(ket_near),
                [True | last, last],
                [own, near, cross_plane, ring, cross_wrap],
                [True | last] * 3 + [last] * 2,
                after=(total,),
            )
            after = (plane_sum,)
    far_first, far_second = products(total)
    sent_far = move(
        far_second, lambda p, s: None if moves_far(p) else (p + half, s)
    )
    sent_down = move(
        jnp.stack([plane_sum, one_late]), lambda p, s: (p - PLANE, s) if p % 2 else None
    )
    totals = jnp.stack(
        [
            jnp.where(last, sent_down[1], one_early),
            jnp.where(upward, sent_down[0], plane_sum),
            jnp.where(stationary, far_first, sent_far),
        ]
    )
    kept_rows = bands // slices

    def part(side):
        return lax.dynamic_slice_in_dim(totals, side * kept_rows, kept_rows, 2)

    done = part(g) + move(part(1 - g), lambda p, s: (p, 1 - s))
    chosen = is_aim[:, :, None, None, None]
    return jnp.sum(jnp.where(chosen, done[None], 0.0), axis=1)[None]


def solution(mesh):
    in_specs = (P("ka", "ga", None, None, None), P("ka", None), P("ka", None), P())
    out_specs = P("ka", None, None, "ga", None)
    return jax.shard_map(step, mesh=mesh, in_specs=in_specs, out_specs=out_specs, check_vma=False)
```
